32 devices in a mesh: curve: 8 (over z, x), level: 4 (over y, core).
Axes of the slice: x: 2, y: 2, z: 4, core: 2. Of those that a mesh axis runs over, the one named last changes fastest.
Arguments:
- right_side: float32 [512, 4096], P(None, ('curve', 'level')), may hold values from -6 to 6
- counts: int32 [32], replicated, may hold values from 96 to 128, as said below
- neighbours: int32 [6, 4096], P(None, ('curve', 'level')), may hold values from -1 to 4095, as said below
Outputs:
- solution: float32 [512, 4096], P(None, ('curve', 'level'))
- residual: float32 [512, 4096], P(None, ('curve', 'level'))
- residual_norm: float32 [], replicated
The draws below stay inside these ranges and needn't reach their ends.
Inputs may be any that keep to these rules, and one draw needn't show every extreme that they name: `counts`: some device holds 128 live bricks and some device holds 96. `neighbours`: A slot's global number is its device times 128 plus its position. The relation is symmetric across opposite faces; padding slots have -1 on every face and no brick names them. Live bricks are numbered along the curve; the brick across face 0, 2 or 4 lies earlier on the curve and the one across face 1, 3 or 5 later, at most 256 live bricks away.
All inputs are finite; a program needn't handle non-finite values.
Results may differ from the reference program's by a relative error of at most 0.00027.
Values sent between devices are 32-bit elements; how exact they have to be, the bound alone decides.
A program may use at most 64 MiB of HBM per device.

```python
import jax
import jax.numpy as jnp
from jax import lax

SLOT_DEV = 128
MIN_LIVE = 96
SIDE = 16
LAYER = 256
CELLS = 512
SLOTS = 4096


def brick_layout(key):
    device_total = SLOTS // SLOT_DEV
    counts = jax.random.randint(jax.random.fold_in(key, 11), (device_total,), MIN_LIVE, SLOT_DEV + 1)
    fullest = jax.random.randint(jax.random.fold_in(key, 12), (), 0, device_total)
    emptiest = (fullest + 1 + jax.random.randint(jax.random.fold_in(key, 13), (), 0, device_total - 1)) % device_total
    device_ids = jnp.arange(device_total)
    counts = jnp.where(device_ids == fullest, SLOT_DEV, counts)
    counts = jnp.where(device_ids == emptiest, MIN_LIVE, counts)
    return counts.astype(jnp.int32)


def morton_split(morton):
    coord_x = jnp.zeros_like(morton)
    coord_y = jnp.zeros_like(morton)
    for bit_index in range(8):
        coord_x = coord_x | (morton >> 2 * bit_index & 1) << bit_index
        coord_y = coord_y | (morton >> 2 * bit_index + 1 & 1) << bit_index
    return (coord_x, coord_y)


def morton_join(coord_x, coord_y):
    morton = jnp.zeros_like(coord_x)
    for bit_index in range(8):
        morton = morton | (coord_x >> bit_index & 1) << 2 * bit_index
        morton = morton | (coord_y >> bit_index & 1) << 2 * bit_index + 1
    return morton


def draw_counts(key, part):
    return brick_layout(key)


def draw_neighbours(key, part):
    counts = brick_layout(key)
    starts = (jnp.cumsum(counts) - counts).astype(jnp.int32)
    total_live = jnp.sum(counts).astype(jnp.int32)
    slot_ids = jnp.arange(SLOTS, dtype=jnp.int32)
    device_of = slot_ids // SLOT_DEV
    offset = slot_ids % SLOT_DEV
    live_slot = offset < counts[device_of]
    live_index = starts[device_of] + offset
    layer_index = live_index // LAYER
    coord_x, coord_y = morton_split(live_index % LAYER)
    columns = []
    for step_x, step_y, step_z in [(-1, 0, 0), (1, 0, 0), (0, -1, 0), (0, 1, 0), (0, 0, -1), (0, 0, 1)]:
        next_x = coord_x + step_x
        next_y = coord_y + step_y
        next_z = layer_index + step_z
        inside = (next_x >= 0) & (next_x < SIDE) & (next_y >= 0) & (next_y < SIDE) & (next_z >= 0)
        other = next_z * LAYER + morton_join(jnp.clip(next_x, 0, SIDE - 1), jnp.clip(next_y, 0, SIDE - 1))
        inside = inside & (other < total_live) & live_slot
        other = jnp.clip(other, 0, total_live - 1)
        owner = (jnp.searchsorted(starts, other, side='right') - 1).astype(jnp.int32)
        global_slot = owner * SLOT_DEV + other - starts[owner]
        columns.append(jnp.where(inside, global_slot, -1))
    return jnp.stack(columns).astype(jnp.int32)


def shard_levels(key, shape, split, least, high):
    loudness = 1.0
    for axis_at, shards_of in split:
        draws = jax.random.uniform(jax.random.fold_in(jax.random.fold_in(key, 6), axis_at), (shards_of,), jnp.float32, least / len(split), high / len(split))
        loudness = loudness * jnp.repeat(jnp.exp(draws), shape[axis_at] // shards_of).reshape((-1,) + (1,) * (len(shape) - 1 - axis_at))
    return loudness


def bell_draw(stream_key, dims, width, limit, pieces=(), kind=jnp.bfloat16):
    drawn = width * jax.random.normal(stream_key, dims, jnp.float32)
    if pieces:
        drawn = drawn * shard_levels(stream_key, dims, pieces, -0.22, 0.18)
    return jnp.clip(drawn, -limit, limit).astype(kind)


def setup_inputs(seed: int = 0) -> dict:
    arg_keys = jax.random.split(jax.random.key(seed), 4)
    right_side = bell_draw(arg_keys[0], (CELLS, SLOTS), 1.0, 6.0, ((1, 32),), jnp.float32)
    counts = draw_counts(jax.random.fold_in(arg_keys[3], 71), 0)
    neighbours = draw_neighbours(jax.random.fold_in(arg_keys[3], 71), 0)
    return {"right_side": right_side, "counts": counts, "neighbours": neighbours}


OPPOSITE = (1, 0, 3, 2, 5, 4)
RELAXATION = 2.0 / 3.0

def brick_faces(values, extent):
    volume = values.reshape(extent, extent, extent, -1)
    surfaces = [volume[0], volume[extent - 1], volume[:, 0], volume[:, extent - 1], volume[:, :, 0], volume[:, :, extent - 1]]
    return jnp.stack([one_face.reshape(extent * extent, -1) for one_face in surfaces])

def gather_ghosts(lookup, position, present):
    ghosts = []
    for face_id in range(6):
        picked = jnp.take(lookup[OPPOSITE[face_id]], position[face_id], axis=1)
        ghosts.append(jnp.where(present[face_id][None, :], picked, jnp.zeros_like(picked)))
    return ghosts

def apply_operator(values, ghosts, extent, weight):
    brick_count = values.shape[1]
    volume = values.reshape(extent, extent, extent, brick_count)
    padded = jnp.pad(volume, ((1, 1), (1, 1), (1, 1), (0, 0)))
    shaped = [ghost.reshape(extent, extent, brick_count) for ghost in ghosts]
    padded = padded.at[0, 1:-1, 1:-1].set(shaped[0])
    padded = padded.at[-1, 1:-1, 1:-1].set(shaped[1])
    padded = padded.at[1:-1, 0, 1:-1].set(shaped[2])
    padded = padded.at[1:-1, -1, 1:-1].set(shaped[3])
    padded = padded.at[1:-1, 1:-1, 0].set(shaped[4])
    padded = padded.at[1:-1, 1:-1, -1].set(shaped[5])
    beside = padded[2:, 1:-1, 1:-1] + padded[:-2, 1:-1, 1:-1]
    beside = beside + padded[1:-1, 2:, 1:-1] + padded[1:-1, :-2, 1:-1]
    beside = beside + padded[1:-1, 1:-1, 2:] + padded[1:-1, 1:-1, :-2]
    return ((6.0 * volume - beside) * weight).reshape(extent * extent * extent, brick_count)

def restrict(values):
    brick_count = values.shape[1]
    grouped = values.reshape(4, 2, 4, 2, 4, 2, brick_count)
    return lax.optimization_barrier(jnp.mean(grouped, axis=(1, 3, 5))).reshape(64, brick_count)

def prolong(coarse):
    brick_count = coarse.shape[1]
    spread = jnp.broadcast_to(coarse.reshape(4, 1, 4, 1, 4, 1, brick_count), (4, 2, 4, 2, 4, 2, brick_count))
    return spread.reshape(512, brick_count)

def precondition(residual_in, exchange):
    relax_fine = RELAXATION / 6.0
    relax_coarse = RELAXATION / 1.5
    sweep_one = relax_fine * residual_in
    sweep_two = sweep_one + relax_fine * (residual_in - apply_operator(sweep_one, exchange(brick_faces(sweep_one, 8)), 8, 1.0))
    defect = residual_in - apply_operator(sweep_two, exchange(brick_faces(sweep_two, 8)), 8, 1.0)
    coarse_rhs = restrict(defect)
    coarse_one = relax_coarse * coarse_rhs
    coarse_two = coarse_one + relax_coarse * (coarse_rhs - apply_operator(coarse_one, exchange(brick_faces(coarse_one, 4)), 4, 0.25))
    sweep_three = sweep_two + prolong(coarse_two)
    return sweep_three + relax_fine * (residual_in - apply_operator(sweep_three, exchange(brick_faces(sweep_three, 8)), 8, 1.0))

def reference(right_side, counts, neighbours):
    slot_ids = jnp.arange(SLOTS, dtype=jnp.int32)
    live_slot = slot_ids % SLOT_DEV < counts[slot_ids // SLOT_DEV]
    residual_in = jnp.where(live_slot[None, :], right_side, jnp.zeros_like(right_side))
    present = neighbours >= 0
    position = jnp.where(present, neighbours, 0).astype(jnp.int32)

    def exchange(surface):
        return gather_ghosts(surface, position, present)
    preconditioned = precondition(residual_in, exchange)
    image = apply_operator(preconditioned, exchange(brick_faces(preconditioned, 8)), 8, 1.0)
    along = jnp.sum(residual_in * preconditioned)
    curvature = jnp.sum(preconditioned * image)
    step_size = along / curvature
    solution = step_size * preconditioned
    residual = residual_in - step_size * image
    residual_norm = jnp.sqrt(jnp.sum(residual * residual))
    return (solution, residual, residual_norm)
```

```python
import functools

import jax
import jax.numpy as jnp
from jax import lax
from jax.experimental import pallas as pl
from jax.experimental.pallas import tpu as pltpu
from jax.sharding import PartitionSpec as P

MIN_LIVE = 96
LAYER = 256
HOPS = 3
AXES = ("curve", "level")
MESH = pl.DeviceIdType.MESH
RELAXATION = 2.0 / 3.0
RELAX_FINE = RELAXATION / 6.0
RELAX_COARSE = RELAXATION / 1.5
F32 = jnp.float32


def kernel(
    sizes,
    stages,
    right_ref,
    counts_ref,
    neighbours_ref,
    solution_ref,
    residual_ref,
    norm_ref,
    source,
    first,
    second,
    image,
    zghost,
    paired,
    coarse,
    shifted,
    faces_fine,
    packed_fine,
    near_fine,
    far_fine,
    faces_coarse,
    packed_coarse,
    near_coarse,
    far_coarse,
    sums,
    send_sems,
    recv_sems,
    sum_send,
    sum_recv,
):
    curve_size, level_size = sizes
    total = curve_size * level_size
    me = lax.axis_index("curve") * level_size + lax.axis_index("level")
    lanes = right_ref.shape[1]
    half = lanes // 2

    def place(index):
        return (index // level_size, index % level_size)

    barrier = pltpu.get_barrier_semaphore()
    greeted = 0
    for size, _, partner in stages:
        for k in range(1, size):
            pl.semaphore_signal(barrier, inc=1, device_id=partner(k), device_id_type=MESH)
            greeted += 1
    direct = len(stages) == 1
    if not direct:
        for hop in range(1, HOPS + 1):
            for sign in (1, -1):
                target = (me + sign * hop + total) % total
                pl.semaphore_signal(barrier, inc=1, device_id=place(target), device_id_type=MESH)
                greeted += 1

    lane = lax.broadcasted_iota(jnp.int32, (1, lanes), 1)
    own_count = counts_ref[me]
    live = lane < own_count
    for x in range(8):
        rows = pl.ds(64 * x, 64)
        value = jnp.where(live, right_ref[rows, :], 0.0)
        source[rows, :] = value
        first[rows, :] = RELAX_FINE * value

    nb = neighbours_ref[...]
    present = nb >= 0
    owner = nb // lanes
    offset = nb % lanes
    face_id = lax.broadcasted_iota(jnp.int32, nb.shape, 0)
    hop_of = jnp.where(face_id % 2 == 0, me - owner, owner - me)
    hop_of = jnp.where(present, hop_of, -1)
    far_count = counts_ref[jnp.maximum(me - HOPS, 0)]
    skipped = jnp.where((face_id % 2 == 0) & (hop_of == HOPS), far_count - half, 0)
    where_at = jnp.clip(offset - skipped, 0, lanes - 1)
    low_half = jnp.broadcast_to(lane < half, (8, lanes))
    tail_index = jnp.broadcast_to(own_count - half + lane % half, (8, lanes))
    head_index = jnp.broadcast_to(lane % half, (8, lanes))

    def pick(block, index):
        rows = block.shape[0]
        return jnp.concatenate(
            [
                jnp.take_along_axis(block[r : r + 8], index, axis=1, mode="promise_in_bounds")
                for r in range(0, rows, 8)
            ],
            axis=0,
        )

    def copy(stage, direction, hop, src, dst):
        sign = 1 if direction == 0 else -1
        target = (me + sign * hop + total) % total
        return pltpu.make_async_remote_copy(
            src_ref=src,
            dst_ref=dst,
            send_sem=send_sems.at[stage, direction, hop - 1],
            recv_sem=recv_sems.at[stage, direction, hop - 1],
            device_id=place(target),
            device_id_type=MESH,
        )

    finishing = []

    def exchange(stage, values, extent, faces, packed, near, far):
        area = extent * extent
        last = extent - 1
        for direction in (0, 1):
            at = last if direction == 0 else 0
            faces[direction, 0:area, :] = values[pl.ds(at * area, area), :]
            for x in range(extent):
                faces[direction, pl.ds(area + x * extent, extent), :] = values[
                    pl.ds(x * area + at * extent, extent), :
                ]
            faces[direction, pl.ds(2 * area, area), :] = values[pl.ds(at, area, extent), :]
            pack = 3 * area // 2
            index = tail_index if direction == 0 else head_index
            for r in range(0, pack, 8):
                a = jnp.take_along_axis(
                    faces[direction, pl.ds(r, 8), :], index, axis=1, mode="promise_in_bounds"
                )
                b = jnp.take_along_axis(
                    faces[direction, pl.ds(pack + r, 8), :], index, axis=1, mode="promise_in_bounds"
                )
                packed[direction, pl.ds(r, 8), :] = jnp.where(low_half, a, b)
        if stage == 0:
            pl.semaphore_wait(barrier, greeted)
        copies = []
        for hop in range(1, HOPS + 1):
            for direction in (0, 1):
                if hop < HOPS:
                    made = copy(stage, direction, hop, faces.at[direction], near.at[direction, hop - 1])
                else:
                    made = copy(stage, direction, hop, packed.at[direction], far.at[direction])
                sends = me + hop < total if direction == 0 else me >= hop
                takes = me >= hop if direction == 0 else me + hop < total
                pl.when(sends)(made.start)
                copies.append((made, takes))
                finishing.append((made, sends))
        for made, takes in copies:
            pl.when(takes)(made.wait_recv)
        ghosts = []
        pack = 3 * area // 2
        for face in range(6):
            direction, slot = face % 2, face // 2
            at = jnp.broadcast_to(where_at[face : face + 1, :], (8, lanes))
            at_high = jnp.minimum(at + half, lanes - 1)
            hops = jnp.broadcast_to(hop_of[face : face + 1, :], (8, lanes))
            pieces = []
            for r in range(0, area, 8):
                row = slot * area + r
                block = jnp.zeros((8, lanes), F32)
                for hop in range(HOPS + 1):
                    index = at
                    if hop == 0:
                        window = faces[direction, pl.ds(row, 8), :]
                    elif hop < HOPS:
                        window = near[direction, hop - 1, pl.ds(row, 8), :]
                    elif row < pack:
                        window = far[direction, pl.ds(row, 8), :]
                    else:
                        window = far[direction, pl.ds(row - pack, 8), :]
                        index = at_high
                    taken = jnp.take_along_axis(window, index, axis=1, mode="promise_in_bounds")
                    block = jnp.where(hops == hop, taken, block)
                pieces.append(block)
            ghosts.append(jnp.concatenate(pieces, axis=0))
        return ghosts

    zrow = lax.broadcasted_iota(jnp.int32, (8, 8, lanes), 1)

    def fine(values, ghosts, use):
        g0, g1, g2, g3, g4, g5 = ghosts
        zghost[pl.ds(0, 64, 8), :] = g4
        zghost[pl.ds(7, 64, 8), :] = g5
        for x in range(8):
            rows = pl.ds(64 * x, 64)
            here = values[rows, :]
            beside = (g0 if x == 0 else values[pl.ds(64 * (x - 1), 64), :]) + (
                g1 if x == 7 else values[pl.ds(64 * (x + 1), 64), :]
            )
            beside = beside + jnp.concatenate([g2[8 * x : 8 * x + 8], here[:-8]], axis=0)
            beside = beside + jnp.concatenate([here[8:], g3[8 * x : 8 * x + 8]], axis=0)
            cube = here.reshape(8, 8, lanes)
            edge = zghost[rows, :].reshape(8, 8, lanes)
            below = jnp.where(zrow == 0, edge, pltpu.roll(cube, 1, 1))
            above = jnp.where(zrow == 7, edge, pltpu.roll(cube, 7, 1))
            beside = beside + (below + above).reshape(64, lanes)
            use(x, rows, here, 6.0 * here - beside)

    def exchange_fine(stage, values):
        return exchange(
            stage,
            values,
            8,
            faces_fine.at[stage],
            packed_fine.at[stage],
            near_fine.at[stage],
            far_fine.at[stage],
        )

    def sweep(x, rows, here, applied):
        second[rows, :] = here + RELAX_FINE * (source[rows, :] - applied)

    fine(first, exchange_fine(0, first), sweep)

    slabs = []

    def restrict(x, rows, here, applied):
        slabs.append(source[rows, :] - applied)
        if x % 2 == 1:
            both = slabs[x - 1] + slabs[x]
            for y in range(4):
                paired[pl.ds(32 * (x // 2) + 8 * y, 8), :] = (
                    both[16 * y : 16 * y + 8] + both[16 * y + 8 : 16 * y + 16]
                )

    fine(second, exchange_fine(1, second), restrict)
    coarse_rhs = 0.125 * (paired[pl.ds(0, 64, 2), :] + paired[pl.ds(1, 64, 2), :])
    coarse_one = RELAX_COARSE * coarse_rhs
    coarse[...] = coarse_one
    g0, g1, g2, g3, g4, g5 = exchange(
        4, coarse, 4, faces_coarse, packed_coarse, near_coarse, far_coarse
    )
    beside = jnp.concatenate([g0, coarse_one[:-16]], axis=0) + jnp.concatenate(
        [coarse_one[16:], g1], axis=0
    )
    for k, shift in enumerate((4, 60, 1, 63)):
        shifted[k, :, :] = pltpu.roll(coarse_one, shift, 0)
    for x in range(4):
        shifted[0, pl.ds(16 * x, 4), :] = g2[4 * x : 4 * x + 4]
        shifted[1, pl.ds(16 * x + 12, 4), :] = g3[4 * x : 4 * x + 4]
    for x in range(4):
        for y in range(4):
            at = 16 * x + 4 * y
            shifted[2, pl.ds(at, 1), :] = g4[4 * x + y : 4 * x + y + 1]
            shifted[3, pl.ds(at + 3, 1), :] = g5[4 * x + y : 4 * x + y + 1]
    beside = beside + (shifted[0] + shifted[1]) + (shifted[2] + shifted[3])
    coarse_two = coarse_one + RELAX_COARSE * (coarse_rhs - 0.25 * (6.0 * coarse_one - beside))
    paired[pl.ds(0, 64, 2), :] = coarse_two
    paired[pl.ds(1, 64, 2), :] = coarse_two
    for x in range(8):
        for y in range(8):
            rows = pl.ds(64 * x + 8 * y, 8)
            second[rows, :] = second[rows, :] + paired[pl.ds(32 * (x // 2) + 8 * (y // 2), 8), :]

    def smooth(x, rows, here, applied):
        first[rows, :] = here + RELAX_FINE * (source[rows, :] - applied)

    fine(second, exchange_fine(2, second), smooth)

    parts = [jnp.zeros((8, lanes), F32)] * 5

    def fold(block):
        return jnp.sum(block.reshape(8, 8, lanes), axis=0)

    def finish(x, rows, here, applied):
        image[rows, :] = applied
        r = source[rows, :]
        for k, term in enumerate((r * here, here * applied, r * r, r * applied, applied * applied)):
            parts[k] = parts[k] + fold(term)

    fine(first, exchange_fine(3, first), finish)

    row = lax.broadcasted_iota(jnp.int32, (8, lanes), 0)
    tile = jnp.zeros((8, lanes), F32)
    for k in range(5):
        tile = jnp.where(row == k, jnp.sum(parts[k], axis=0, keepdims=True), tile)
    base = 0
    for size, mine, partner in stages:
        sums[base + mine] = tile
        copies = []
        for k in range(1, size):
            made = pltpu.make_async_remote_copy(
                src_ref=sums.at[base + mine],
                dst_ref=sums.at[base + mine],
                send_sem=sum_send.at[base + k],
                recv_sem=sum_recv.at[base + k],
                device_id=partner(k),
                device_id_type=MESH,
            )
            made.start()
            copies.append(made)
        for made in copies:
            made.wait_recv()
        tile = jnp.sum(sums[base : base + size], axis=0)
        for made in copies:
            made.wait_send()
        base += size
    whole = jnp.sum(tile, axis=1, keepdims=True)
    along, curvature, old_square, cross, image_square = [whole[k : k + 1] for k in range(5)]
    step = along / curvature
    square = old_square - 2.0 * step * cross + step * step * image_square
    norm_ref[...] = jnp.broadcast_to(jnp.sqrt(square), norm_ref.shape)
    for x in range(8):
        rows = pl.ds(64 * x, 64)
        solution_ref[rows, :] = step * first[rows, :]
        residual_ref[rows, :] = source[rows, :] - step * image[rows, :]
    for made, sends in finishing:
        pl.when(sends)(made.wait_send)


def local(sizes, right_side, counts, neighbours):
    cells, lanes = right_side.shape
    curve_size, level_size = sizes
    total = curve_size * level_size

    def body(*refs):
        curve, level = lax.axis_index("curve"), lax.axis_index("level")
        if total <= 64:
            me = curve * level_size + level

            def everyone(k):
                other = (me + k) % total
                return (other // level_size, other % level_size)

            stages = [(total, me, everyone)]
        else:
            stages = [
                (level_size, level, lambda k: (curve, (level + k) % level_size)),
                (curve_size, curve, lambda k: ((curve + k) % curve_size, level)),
            ]
        kernel(sizes, stages, *refs)

    sum_rows = total if total <= 64 else curve_size + level_size
    vmem = pl.BlockSpec(memory_space=pltpu.VMEM)
    block = jax.ShapeDtypeStruct((cells, lanes), F32)
    out = pl.pallas_call(
        body,
        out_shape=(block, block, jax.ShapeDtypeStruct((8, lanes), F32)),
        in_specs=[vmem, pl.BlockSpec(memory_space=pltpu.SMEM), vmem],
        out_specs=(vmem, vmem, vmem),
        scratch_shapes=[
            pltpu.VMEM((cells, lanes), F32),
            pltpu.VMEM((cells, lanes), F32),
            pltpu.VMEM((cells, lanes), F32),
            pltpu.VMEM((cells, lanes), F32),
            pltpu.VMEM((cells, lanes), F32),
            pltpu.VMEM((cells // 4, lanes), F32),
            pltpu.VMEM((cells // 8, lanes), F32),
            pltpu.VMEM((4, cells // 8, lanes), F32),
            pltpu.VMEM((4, 2, 192, lanes), F32),
            pltpu.VMEM((4, 2, 96, lanes), F32),
            pltpu.VMEM((4, 2, 2, 192, lanes), F32),
            pltpu.VMEM((4, 2, 96, lanes), F32),
            pltpu.VMEM((2, 48, lanes), F32),
            pltpu.VMEM((2, 24, lanes), F32),
            pltpu.VMEM((2, 2, 48, lanes), F32),
            pltpu.VMEM((2, 24, lanes), F32),
            pltpu.VMEM((sum_rows, 8, lanes), F32),
            pltpu.SemaphoreType.DMA((5, 2, HOPS)),
            pltpu.SemaphoreType.DMA((5, 2, HOPS)),
            pltpu.SemaphoreType.DMA((sum_rows,)),
            pltpu.SemaphoreType.DMA((sum_rows,)),
        ],
        compiler_params=pltpu.CompilerParams(collective_id=0, has_side_effects=True),
    )(right_side, counts, neighbours)
    return out[0], out[1], out[2][0, 0]


def solution(mesh):
    sizes = tuple(mesh.shape[name] for name in AXES)
    in_specs = (P(None, AXES), P(), P(None, AXES))
    out_specs = (P(None, AXES), P(None, AXES), P())
    return jax.shard_map(
        functools.partial(local, sizes), mesh=mesh, in_specs=in_specs, out_specs=out_specs, check_vma=False
    )
```

```python
import functools

import jax
import jax.numpy as jnp
from jax import lax
from jax.experimental import pallas as pl
from jax.experimental.pallas import tpu as pltpu
from jax.sharding import PartitionSpec as P

MIN_LIVE = 96
LAYER = 256
HOPS = 3
AXES = ("curve", "level")
MESH = pl.DeviceIdType.MESH
RELAXATION = 2.0 / 3.0
RELAX_FINE = RELAXATION / 6.0
RELAX_COARSE = RELAXATION / 1.5
F32 = jnp.float32


def kernel(
    sizes,
    stages,
    right_ref,
    counts_ref,
    neighbours_ref,
    solution_ref,
    residual_ref,
    norm_ref,
    source,
    first,
    second,
    image,
    zghost,
    paired,
    coarse,
    shifted,
    doubled,
    faces_fine,
    packed_fine,
    near_fine,
    far_fine,
    faces_coarse,
    packed_coarse,
    near_coarse,
    far_coarse,
    sums,
    send_sems,
    recv_sems,
    sum_send,
    sum_recv,
):
    curve_size, level_size = sizes
    total = curve_size * level_size
    me = lax.axis_index("curve") * level_size + lax.axis_index("level")
    lanes = right_ref.shape[1]
    half = lanes // 2

    def place(index):
        return (index // level_size, index % level_size)

    barrier = pltpu.get_barrier_semaphore()
    greeted = 0
    for size, _, partner in stages:
        for k in range(1, size):
            pl.semaphore_signal(barrier, inc=1, device_id=partner(k), device_id_type=MESH)
            greeted += 1
    direct = len(stages) == 1
    if not direct:
        for hop in range(1, HOPS + 1):
            for sign in (1, -1):
                target = (me + sign * hop + total) % total
                pl.semaphore_signal(barrier, inc=1, device_id=place(target), device_id_type=MESH)
                greeted += 1

    lane = lax.broadcasted_iota(jnp.int32, (1, lanes), 1)
    own_count = counts_ref[me]
    live = lane < own_count
    for x in range(8):
        rows = pl.ds(64 * x, 64)
        value = jnp.where(live, right_ref[rows, :], 0.0)
        source[rows, :] = value
        first[rows, :] = RELAX_FINE * value

    nb = neighbours_ref[...]
    present = nb >= 0
    owner = nb // lanes
    offset = nb % lanes
    face_id = lax.broadcasted_iota(jnp.int32, nb.shape, 0)
    hop_of = jnp.where(face_id % 2 == 0, me - owner, owner - me)
    hop_of = jnp.where(present, hop_of, -1)
    far_count = counts_ref[jnp.maximum(me - HOPS, 0)]
    skipped = jnp.where((face_id % 2 == 0) & (hop_of == HOPS), far_count - half, 0)
    where_at = jnp.clip(offset - skipped, 0, lanes - 1)
    low_half = jnp.broadcast_to(lane < half, (8, lanes))
    tail_index = jnp.broadcast_to(own_count - half + lane % half, (8, lanes))
    head_index = jnp.broadcast_to(lane % half, (8, lanes))

    def pick(block, index):
        rows = block.shape[0]
        return jnp.concatenate(
            [
                jnp.take_along_axis(block[r : r + 8], index, axis=1, mode="promise_in_bounds")
                for r in range(0, rows, 8)
            ],
            axis=0,
        )

    def copy(stage, direction, hop, src, dst):
        sign = 1 if direction == 0 else -1
        target = (me + sign * hop + total) % total
        return pltpu.make_async_remote_copy(
            src_ref=src,
            dst_ref=dst,
            send_sem=send_sems.at[stage, direction, hop - 1],
            recv_sem=recv_sems.at[stage, direction, hop - 1],
            device_id=place(target),
            device_id_type=MESH,
        )

    finishing = []

    def exchange(stage, values, extent, faces, packed, near, far):
        area = extent * extent
        last = extent - 1
        for direction in (0, 1):
            at = last if direction == 0 else 0
            faces[direction, 0:area, :] = values[pl.ds(at * area, area), :]
            for x in range(extent):
                faces[direction, pl.ds(area + x * extent, extent), :] = values[
                    pl.ds(x * area + at * extent, extent), :
                ]
            faces[direction, pl.ds(2 * area, area), :] = values[pl.ds(at, area, extent), :]
            pack = 3 * area // 2
            index = tail_index if direction == 0 else head_index
            for r in range(0, pack, 8):
                a = jnp.take_along_axis(
                    faces[direction, pl.ds(r, 8), :], index, axis=1, mode="promise_in_bounds"
                )
                b = jnp.take_along_axis(
                    faces[direction, pl.ds(pack + r, 8), :], index, axis=1, mode="promise_in_bounds"
                )
                packed[direction, pl.ds(r, 8), :] = jnp.where(low_half, a, b)
        if stage == 0:
            pl.semaphore_wait(barrier, greeted)
        copies = []
        for hop in range(1, HOPS + 1):
            for direction in (0, 1):
                if hop < HOPS:
                    made = copy(stage, direction, hop, faces.at[direction], near.at[direction, hop - 1])
                else:
                    made = copy(stage, direction, hop, packed.at[direction], far.at[direction])
                sends = me + hop < total if direction == 0 else me >= hop
                takes = me >= hop if direction == 0 else me + hop < total
                pl.when(sends)(made.start)
                copies.append((made, takes))
                finishing.append((made, sends))
        for made, takes in copies:
            pl.when(takes)(made.wait_recv)
        ghosts = []
        pack = 3 * area // 2
        for face in range(6):
            direction, slot = face % 2, face // 2
            at = jnp.broadcast_to(where_at[face : face + 1, :], (8, lanes))
            at_high = jnp.minimum(at + half, lanes - 1)
            hops = jnp.broadcast_to(hop_of[face : face + 1, :], (8, lanes))
            pieces = []
            for r in range(0, area, 8):
                row = slot * area + r
                block = jnp.zeros((8, lanes), F32)
                for hop in range(HOPS + 1):
                    index = at
                    if hop == 0:
                        window = faces[direction, pl.ds(row, 8), :]
                    elif hop < HOPS:
                        window = near[direction, hop - 1, pl.ds(row, 8), :]
                    elif row < pack:
                        window = far[direction, pl.ds(row, 8), :]
                    else:
                        window = far[direction, pl.ds(row - pack, 8), :]
                        index = at_high
                    taken = jnp.take_along_axis(window, index, axis=1, mode="promise_in_bounds")
                    block = jnp.where(hops == hop, taken, block)
                pieces.append(block)
            ghosts.append(jnp.concatenate(pieces, axis=0))
        return ghosts

    zrow = lax.broadcasted_iota(jnp.int32, (8, 8, lanes), 1)

    def fine(values, ghosts, use):
        g0, g1, g2, g3, g4, g5 = ghosts
        zghost[pl.ds(0, 64, 8), :] = g4
        zghost[pl.ds(7, 64, 8), :] = g5
        for x in range(8):
            rows = pl.ds(64 * x, 64)
            here = values[rows, :]
            beside = (g0 if x == 0 else values[pl.ds(64 * (x - 1), 64), :]) + (
                g1 if x == 7 else values[pl.ds(64 * (x + 1), 64), :]
            )
            beside = beside + jnp.concatenate([g2[8 * x : 8 * x + 8], here[:-8]], axis=0)
            beside = beside + jnp.concatenate([here[8:], g3[8 * x : 8 * x + 8]], axis=0)
            cube = here.reshape(8, 8, lanes)
            edge = zghost[rows, :].reshape(8, 8, lanes)
            below = jnp.where(zrow == 0, edge, pltpu.roll(cube, 1, 1))
            above = jnp.where(zrow == 7, edge, pltpu.roll(cube, 7, 1))
            beside = beside + (below + above).reshape(64, lanes)
            use(x, rows, here, 6.0 * here - beside)

    def exchange_fine(stage, k, values):
        return exchange(
            stage, values, 8, faces_fine.at[k], packed_fine.at[k], near_fine.at[k], far_fine.at[k]
        )

    def exchange_coarse(stage, k):
        return exchange(
            stage,
            coarse,
            4,
            faces_coarse.at[k],
            packed_coarse.at[k],
            near_coarse.at[k],
            far_coarse.at[k],
        )

    def sweep(x, rows, here, applied):
        second[rows, :] = here + RELAX_FINE * (source[rows, :] - applied)

    fine(first, exchange_fine(0, 0, first), sweep)

    slabs = []

    def restrict(x, rows, here, applied):
        slabs.append(source[rows, :] - applied)
        if x % 2 == 1:
            both = slabs[x - 1] + slabs[x]
            for y in range(4):
                paired[pl.ds(32 * (x // 2) + 8 * y, 8), :] = (
                    both[16 * y : 16 * y + 8] + both[16 * y + 8 : 16 * y + 16]
                )

    ghosts = exchange_fine(1, 1, second)
    fine(second, ghosts, restrict)
    coarse_rhs = 0.125 * (paired[pl.ds(0, 64, 2), :] + paired[pl.ds(1, 64, 2), :])
    coarse_one = RELAX_COARSE * coarse_rhs
    coarse[...] = coarse_one
    g0, g1, g2, g3, g4, g5 = exchange_coarse(2, 0)
    beside = jnp.concatenate([g0, coarse_one[:-16]], axis=0) + jnp.concatenate(
        [coarse_one[16:], g1], axis=0
    )
    for k, shift in enumerate((4, 60, 1, 63)):
        shifted[k, :, :] = pltpu.roll(coarse_one, shift, 0)
    for x in range(4):
        shifted[0, pl.ds(16 * x, 4), :] = g2[4 * x : 4 * x + 4]
        shifted[1, pl.ds(16 * x + 12, 4), :] = g3[4 * x : 4 * x + 4]
    for x in range(4):
        for y in range(4):
            at = 16 * x + 4 * y
            shifted[2, pl.ds(at, 1), :] = g4[4 * x + y : 4 * x + y + 1]
            shifted[3, pl.ds(at + 3, 1), :] = g5[4 * x + y : 4 * x + y + 1]
    beside = beside + (shifted[0] + shifted[1]) + (shifted[2] + shifted[3])
    coarse_two = coarse_one + RELAX_COARSE * (coarse_rhs - 0.25 * (6.0 * coarse_one - beside))
    coarse[...] = coarse_two
    paired[pl.ds(0, 64, 2), :] = coarse_two
    paired[pl.ds(1, 64, 2), :] = coarse_two
    for x in range(8):
        for y in range(8):
            rows = pl.ds(64 * x + 8 * y, 8)
            second[rows, :] = second[rows, :] + paired[pl.ds(32 * (x // 2) + 8 * (y // 2), 8), :]

    corrections = exchange_coarse(3, 1)
    for face in range(6):
        doubled[face, pl.ds(0, 16, 2), :] = corrections[face]
        doubled[face, pl.ds(1, 16, 2), :] = corrections[face]
        ghosts[face] = ghosts[face] + jnp.concatenate(
            [doubled[face, pl.ds(8 * (a // 2), 8), :] for a in range(8)], axis=0
        )

    def smooth(x, rows, here, applied):
        first[rows, :] = here + RELAX_FINE * (source[rows, :] - applied)

    fine(second, ghosts, smooth)

    parts = [jnp.zeros((8, lanes), F32)] * 5

    def fold(block):
        return jnp.sum(block.reshape(8, 8, lanes), axis=0)

    def finish(x, rows, here, applied):
        image[rows, :] = applied
        r = source[rows, :]
        for k, term in enumerate((r * here, here * applied, r * r, r * applied, applied * applied)):
            parts[k] = parts[k] + fold(term)

    fine(first, exchange_fine(4, 2, first), finish)

    row = lax.broadcasted_iota(jnp.int32, (8, lanes), 0)
    tile = jnp.zeros((8, lanes), F32)
    for k in range(5):
        tile = jnp.where(row == k, jnp.sum(parts[k], axis=0, keepdims=True), tile)
    base = 0
    for size, mine, partner in stages:
        sums[base + mine] = tile
        copies = []
        for k in range(1, size):
            made = pltpu.make_async_remote_copy(
                src_ref=sums.at[base + mine],
                dst_ref=sums.at[base + mine],
                send_sem=sum_send.at[base + k],
                recv_sem=sum_recv.at[base + k],
                device_id=partner(k),
                device_id_type=MESH,
            )
            made.start()
            copies.append(made)
        for made in copies:
            made.wait_recv()
        tile = jnp.sum(sums[base : base + size], axis=0)
        for made in copies:
            made.wait_send()
        base += size
    whole = jnp.sum(tile, axis=1, keepdims=True)
    along, curvature, old_square, cross, image_square = [whole[k : k + 1] for k in range(5)]
    step = along / curvature
    square = old_square - 2.0 * step * cross + step * step * image_square
    norm_ref[...] = jnp.broadcast_to(jnp.sqrt(square), norm_ref.shape)
    for x in range(8):
        rows = pl.ds(64 * x, 64)
        solution_ref[rows, :] = step * first[rows, :]
        residual_ref[rows, :] = source[rows, :] - step * image[rows, :]
    for made, sends in finishing:
        pl.when(sends)(made.wait_send)


def local(sizes, right_side, counts, neighbours):
    cells, lanes = right_side.shape
    curve_size, level_size = sizes
    total = curve_size * level_size

    def body(*refs):
        curve, level = lax.axis_index("curve"), lax.axis_index("level")
        if total <= 64:
            me = curve * level_size + level

            def everyone(k):
                other = (me + k) % total
                return (other // level_size, other % level_size)

            stages = [(total, me, everyone)]
        else:
            stages = [
                (level_size, level, lambda k: (curve, (level + k) % level_size)),
                (curve_size, curve, lambda k: ((curve + k) % curve_size, level)),
            ]
        kernel(sizes, stages, *refs)

    sum_rows = total if total <= 64 else curve_size + level_size
    vmem = pl.BlockSpec(memory_space=pltpu.VMEM)
    block = jax.ShapeDtypeStruct((cells, lanes), F32)
    out = pl.pallas_call(
        body,
        out_shape=(block, block, jax.ShapeDtypeStruct((8, lanes), F32)),
        in_specs=[vmem, pl.BlockSpec(memory_space=pltpu.SMEM), vmem],
        out_specs=(vmem, vmem, vmem),
        scratch_shapes=[
            pltpu.VMEM((cells, lanes), F32),
            pltpu.VMEM((cells, lanes), F32),
            pltpu.VMEM((cells, lanes), F32),
            pltpu.VMEM((cells, lanes), F32),
            pltpu.VMEM((cells, lanes), F32),
            pltpu.VMEM((cells // 4, lanes), F32),
            pltpu.VMEM((cells // 8, lanes), F32),
            pltpu.VMEM((4, cells // 8, lanes), F32),
            pltpu.VMEM((6, 32, lanes), F32),
            pltpu.VMEM((3, 2, 192, lanes), F32),
            pltpu.VMEM((3, 2, 96, lanes), F32),
            pltpu.VMEM((3, 2, 2, 192, lanes), F32),
            pltpu.VMEM((3, 2, 96, lanes), F32),
            pltpu.VMEM((2, 2, 48, lanes), F32),
            pltpu.VMEM((2, 2, 24, lanes), F32),
            pltpu.VMEM((2, 2, 2, 48, lanes), F32),
            pltpu.VMEM((2, 2, 24, lanes), F32),
            pltpu.VMEM((sum_rows, 8, lanes), F32),
            pltpu.SemaphoreType.DMA((5, 2, HOPS)),
            pltpu.SemaphoreType.DMA((5, 2, HOPS)),
            pltpu.SemaphoreType.DMA((sum_rows,)),
            pltpu.SemaphoreType.DMA((sum_rows,)),
        ],
        compiler_params=pltpu.CompilerParams(collective_id=0, has_side_effects=True),
    )(right_side, counts, neighbours)
    return out[0], out[1], out[2][0, 0]


def solution(mesh):
    sizes = tuple(mesh.shape[name] for name in AXES)
    in_specs = (P(None, AXES), P(), P(None, AXES))
    out_specs = (P(None, AXES), P(None, AXES), P())
    return jax.shard_map(
        functools.partial(local, sizes), mesh=mesh, in_specs=in_specs, out_specs=out_specs, check_vma=False
    )
```

```python
import functools

import jax
import jax.numpy as jnp
from jax import lax
from jax.experimental import pallas as pl
from jax.experimental.pallas import tpu as pltpu
from jax.sharding import PartitionSpec as P

MIN_LIVE = 96
LAYER = 256
HOPS = 3
AXES = ("curve", "level")
MESH = pl.DeviceIdType.MESH
RELAXATION = 2.0 / 3.0
RELAX_FINE = RELAXATION / 6.0
RELAX_COARSE = RELAXATION / 1.5
F32 = jnp.float32


def kernel(
    sizes,
    stages,
    right_ref,
    counts_ref,
    neighbours_ref,
    solution_ref,
    residual_ref,
    norm_ref,
    source,
    first,
    second,
    image,
    zghost,
    paired,
    coarse,
    shifted,
    doubled,
    faces_fine,
    packed_fine,
    windows_fine,
    faces_coarse,
    packed_coarse,
    windows_coarse,
    sums,
    *sems,
):
    link_sems, relay_sems, pair_sems, far_sems, (sum_send, sum_recv) = [
        sems[i : i + 2] for i in range(0, 10, 2)
    ]
    curve_size, level_size = sizes
    total = curve_size * level_size
    me = lax.axis_index("curve") * level_size + lax.axis_index("level")
    lanes = right_ref.shape[1]
    half = lanes // 2

    def place(index):
        return (index // level_size, index % level_size)

    barrier = pltpu.get_barrier_semaphore()
    greeted = 0
    for size, _, peer in stages:
        for k in range(1, size):
            pl.semaphore_signal(barrier, inc=1, device_id=peer(k), device_id_type=MESH)
            greeted += 1
    direct = len(stages) == 1
    if not direct:
        for hop in range(1, HOPS + 1):
            for sign in (1, -1):
                target = (me + sign * hop + total) % total
                pl.semaphore_signal(barrier, inc=1, device_id=place(target), device_id_type=MESH)
                greeted += 1

    lane = lax.broadcasted_iota(jnp.int32, (1, lanes), 1)
    own_count = counts_ref[me]
    live = lane < own_count
    for x in range(8):
        rows = pl.ds(64 * x, 64)
        value = jnp.where(live, right_ref[rows, :], 0.0)
        source[rows, :] = value
        first[rows, :] = RELAX_FINE * value

    nb = neighbours_ref[...]
    present = nb >= 0
    owner = nb // lanes
    offset = nb % lanes
    face_id = lax.broadcasted_iota(jnp.int32, nb.shape, 0)
    hop_of = jnp.where(face_id % 2 == 0, me - owner, owner - me)
    hop_of = jnp.where(present, hop_of, -1)
    far_count = counts_ref[jnp.maximum(me - HOPS, 0)]
    odd = me % 2
    even = 1 - odd
    partner = me + 1 - 2 * odd
    earlier_pair = me >= 2
    later_pair = me - odd + 2 < total
    reaches = (1 + 2 * even, 1 + 2 * odd)
    arrives = (2 * odd, 2 * even)
    far_there = jnp.where(odd == 1, me + HOPS < total, me >= HOPS)
    far_device = (me + HOPS * (2 * odd - 1) + total) % total
    skipped = jnp.where(
        (face_id % 2 == 0) & (hop_of == HOPS), even * (far_count - half), 0
    )
    where_at = jnp.clip(offset - skipped, 0, lanes - 1)
    low_half = jnp.broadcast_to(lane < half, (8, lanes))
    pack_index = jnp.broadcast_to(odd * (own_count - half) + lane % half, (8, lanes))

    def pick(block, index):
        return jnp.take_along_axis(block, index, axis=1, mode="promise_in_bounds")

    finishing = []

    def send(src, dst, sems, at, target, sends):
        made = pltpu.make_async_remote_copy(
            src_ref=src,
            dst_ref=dst,
            send_sem=sems[0].at[at],
            recv_sem=sems[1].at[at],
            device_id=place(target),
            device_id_type=MESH,
        )
        finishing.append((made, sends))
        return made

    def exchange(stage, values, extent, faces, packed, windows):
        area = extent * extent
        last = extent - 1
        pack = 3 * area // 2
        for direction in (0, 1):
            at = last if direction == 0 else 0
            faces[direction, 0:area, :] = values[pl.ds(at * area, area), :]
            for x in range(extent):
                faces[direction, pl.ds(area + x * extent, extent), :] = values[
                    pl.ds(x * area + at * extent, extent), :
                ]
            faces[direction, pl.ds(2 * area, area), :] = values[pl.ds(at, area, extent), :]
        if stage == 0:
            pl.semaphore_wait(barrier, greeted)
        links = []
        for chunk in range(3):
            rows = pl.ds(chunk * area, area)
            for direction in (0, 1):
                reach = reaches[direction]
                target = me + reach if direction == 0 else me - reach
                made = send(
                    faces.at[direction, rows],
                    windows.at[direction, reach - 1, rows],
                    link_sems,
                    (stage, direction, chunk),
                    (target + total) % total,
                    later_pair if direction == 0 else earlier_pair,
                )
                pl.when(later_pair if direction == 0 else earlier_pair)(made.start)
                links.append((direction, chunk, rows, made))
        inside = send(faces.at[odd], windows.at[odd, 0], pair_sems, (stage,), partner, None)
        inside.start()
        for r in range(0, pack, 8):
            a = pick(faces[1 - odd, pl.ds(r, 8), :], pack_index)
            b = pick(faces[1 - odd, pl.ds(pack + r, 8), :], pack_index)
            packed[pl.ds(r, 8), :] = jnp.where(low_half, a, b)
        far = send(
            packed, windows.at[1 - odd, 2, pl.ds(0, pack)], far_sems, (stage,), far_device, far_there
        )
        pl.when(far_there)(far.start)
        relays = []
        for direction, chunk, rows, made in links:
            comes = earlier_pair if direction == 0 else later_pair
            relay = send(
                windows.at[direction, arrives[direction], rows],
                windows.at[direction, 1, rows],
                relay_sems,
                (stage, direction, chunk),
                partner,
                comes,
            )

            @pl.when(comes)
            def _():
                made.wait_recv()
                relay.start()

            relays.append((relay, comes))
        inside.wait_recv()
        pl.when(far_there)(far.wait_recv)
        for relay, comes in relays:
            pl.when(comes)(relay.wait_recv)
        ghosts = []
        for face in range(6):
            direction, slot = face % 2, face // 2
            at = jnp.broadcast_to(where_at[face : face + 1, :], (8, lanes))
            is_packed = odd == direction
            at_high = jnp.where(is_packed, jnp.minimum(at + half, lanes - 1), at)
            hops = jnp.broadcast_to(hop_of[face : face + 1, :], (8, lanes))
            pieces = []
            for r in range(0, area, 8):
                row = slot * area + r
                block = jnp.zeros((8, lanes), F32)
                for hop in range(HOPS + 1):
                    index = at
                    if hop == 0:
                        window = faces[direction, pl.ds(row, 8), :]
                    elif hop < HOPS or row < pack:
                        window = windows[direction, hop - 1, pl.ds(row, 8), :]
                    else:
                        start = pl.multiple_of(row - jnp.where(is_packed, pack, 0), 8)
                        window = windows[direction, hop - 1, pl.ds(start, 8), :]
                        index = at_high
                    block = jnp.where(hops == hop, pick(window, index), block)
                pieces.append(block)
            ghosts.append(jnp.concatenate(pieces, axis=0))
        return ghosts

    zrow = lax.broadcasted_iota(jnp.int32, (8, 8, lanes), 1)

    def fine(values, ghosts, use):
        g0, g1, g2, g3, g4, g5 = ghosts
        zghost[pl.ds(0, 64, 8), :] = g4
        zghost[pl.ds(7, 64, 8), :] = g5
        for x in range(8):
            rows = pl.ds(64 * x, 64)
            here = values[rows, :]
            beside = (g0 if x == 0 else values[pl.ds(64 * (x - 1), 64), :]) + (
                g1 if x == 7 else values[pl.ds(64 * (x + 1), 64), :]
            )
            beside = beside + jnp.concatenate([g2[8 * x : 8 * x + 8], here[:-8]], axis=0)
            beside = beside + jnp.concatenate([here[8:], g3[8 * x : 8 * x + 8]], axis=0)
            cube = here.reshape(8, 8, lanes)
            edge = zghost[rows, :].reshape(8, 8, lanes)
            below = jnp.where(zrow == 0, edge, pltpu.roll(cube, 1, 1))
            above = jnp.where(zrow == 7, edge, pltpu.roll(cube, 7, 1))
            beside = beside + (below + above).reshape(64, lanes)
            use(x, rows, here, 6.0 * here - beside)

    def exchange_fine(stage, k, values):
        return exchange(
            stage, values, 8, faces_fine.at[k], packed_fine.at[k], windows_fine.at[k]
        )

    def exchange_coarse(stage, k):
        return exchange(
            stage, coarse, 4, faces_coarse.at[k], packed_coarse.at[k], windows_coarse.at[k]
        )

    def sweep(x, rows, here, applied):
        second[rows, :] = here + RELAX_FINE * (source[rows, :] - applied)

    fine(first, exchange_fine(0, 0, first), sweep)

    slabs = []

    def restrict(x, rows, here, applied):
        slabs.append(source[rows, :] - applied)
        if x % 2 == 1:
            both = slabs[x - 1] + slabs[x]
            for y in range(4):
                paired[pl.ds(32 * (x // 2) + 8 * y, 8), :] = (
                    both[16 * y : 16 * y + 8] + both[16 * y + 8 : 16 * y + 16]
                )

    ghosts = exchange_fine(1, 1, second)
    fine(second, ghosts, restrict)
    coarse_rhs = 0.125 * (paired[pl.ds(0, 64, 2), :] + paired[pl.ds(1, 64, 2), :])
    coarse_one = RELAX_COARSE * coarse_rhs
    coarse[...] = coarse_one
    g0, g1, g2, g3, g4, g5 = exchange_coarse(2, 0)
    beside = jnp.concatenate([g0, coarse_one[:-16]], axis=0) + jnp.concatenate(
        [coarse_one[16:], g1], axis=0
    )
    for k, shift in enumerate((4, 60, 1, 63)):
        shifted[k, :, :] = pltpu.roll(coarse_one, shift, 0)
    for x in range(4):
        shifted[0, pl.ds(16 * x, 4), :] = g2[4 * x : 4 * x + 4]
        shifted[1, pl.ds(16 * x + 12, 4), :] = g3[4 * x : 4 * x + 4]
    for x in range(4):
        for y in range(4):
            at = 16 * x + 4 * y
            shifted[2, pl.ds(at, 1), :] = g4[4 * x + y : 4 * x + y + 1]
            shifted[3, pl.ds(at + 3, 1), :] = g5[4 * x + y : 4 * x + y + 1]
    beside = beside + (shifted[0] + shifted[1]) + (shifted[2] + shifted[3])
    coarse_two = coarse_one + RELAX_COARSE * (coarse_rhs - 0.25 * (6.0 * coarse_one - beside))
    coarse[...] = coarse_two
    paired[pl.ds(0, 64, 2), :] = coarse_two
    paired[pl.ds(1, 64, 2), :] = coarse_two
    for x in range(8):
        for y in range(8):
            rows = pl.ds(64 * x + 8 * y, 8)
            second[rows, :] = second[rows, :] + paired[pl.ds(32 * (x // 2) + 8 * (y // 2), 8), :]

    corrections = exchange_coarse(3, 1)
    for face in range(6):
        doubled[face, pl.ds(0, 16, 2), :] = corrections[face]
        doubled[face, pl.ds(1, 16, 2), :] = corrections[face]
        ghosts[face] = ghosts[face] + jnp.concatenate(
            [doubled[face, pl.ds(8 * (a // 2), 8), :] for a in range(8)], axis=0
        )

    def smooth(x, rows, here, applied):
        first[rows, :] = here + RELAX_FINE * (source[rows, :] - applied)

    fine(second, ghosts, smooth)

    parts = [jnp.zeros((8, lanes), F32)] * 5

    def fold(block):
        return jnp.sum(block.reshape(8, 8, lanes), axis=0)

    def finish(x, rows, here, applied):
        image[rows, :] = applied
        r = source[rows, :]
        for k, term in enumerate((r * here, here * applied, r * r, r * applied, applied * applied)):
            parts[k] = parts[k] + fold(term)

    fine(first, exchange_fine(4, 2, first), finish)

    row = lax.broadcasted_iota(jnp.int32, (8, lanes), 0)
    tile = jnp.zeros((8, lanes), F32)
    for k in range(5):
        tile = jnp.where(row == k, jnp.sum(parts[k], axis=0, keepdims=True), tile)
    base = 0
    for size, mine, peer in stages:
        sums[base + mine] = tile
        copies = []
        for k in range(1, size):
            made = pltpu.make_async_remote_copy(
                src_ref=sums.at[base + mine],
                dst_ref=sums.at[base + mine],
                send_sem=sum_send.at[base + k],
                recv_sem=sum_recv.at[base + k],
                device_id=peer(k),
                device_id_type=MESH,
            )
            made.start()
            copies.append(made)
        for made in copies:
            made.wait_recv()
        tile = jnp.sum(sums[base : base + size], axis=0)
        for made in copies:
            made.wait_send()
        base += size
    whole = jnp.sum(tile, axis=1, keepdims=True)
    along, curvature, old_square, cross, image_square = [whole[k : k + 1] for k in range(5)]
    step = along / curvature
    square = old_square - 2.0 * step * cross + step * step * image_square
    norm_ref[...] = jnp.broadcast_to(jnp.sqrt(square), norm_ref.shape)
    for x in range(8):
        rows = pl.ds(64 * x, 64)
        solution_ref[rows, :] = step * first[rows, :]
        residual_ref[rows, :] = source[rows, :] - step * image[rows, :]
    for made, sends in finishing:
        if sends is None:
            made.wait_send()
        else:
            pl.when(sends)(made.wait_send)


def local(sizes, right_side, counts, neighbours):
    cells, lanes = right_side.shape
    curve_size, level_size = sizes
    total = curve_size * level_size

    def body(*refs):
        curve, level = lax.axis_index("curve"), lax.axis_index("level")
        if total <= 64:
            me = curve * level_size + level

            def everyone(k):
                other = (me + k) % total
                return (other // level_size, other % level_size)

            stages = [(total, me, everyone)]
        else:
            stages = [
                (level_size, level, lambda k: (curve, (level + k) % level_size)),
                (curve_size, curve, lambda k: ((curve + k) % curve_size, level)),
            ]
        kernel(sizes, stages, *refs)

    sum_rows = total if total <= 64 else curve_size + level_size
    vmem = pl.BlockSpec(memory_space=pltpu.VMEM)
    block = jax.ShapeDtypeStruct((cells, lanes), F32)
    out = pl.pallas_call(
        body,
        out_shape=(block, block, jax.ShapeDtypeStruct((8, lanes), F32)),
        in_specs=[vmem, pl.BlockSpec(memory_space=pltpu.SMEM), vmem],
        out_specs=(vmem, vmem, vmem),
        scratch_shapes=[
            pltpu.VMEM((cells, lanes), F32),
            pltpu.VMEM((cells, lanes), F32),
            pltpu.VMEM((cells, lanes), F32),
            pltpu.VMEM((cells, lanes), F32),
            pltpu.VMEM((cells, lanes), F32),
            pltpu.VMEM((cells // 4, lanes), F32),
            pltpu.VMEM((cells // 8, lanes), F32),
            pltpu.VMEM((4, cells // 8, lanes), F32),
            pltpu.VMEM((6, 32, lanes), F32),
            pltpu.VMEM((3, 2, 192, lanes), F32),
            pltpu.VMEM((3, 96, lanes), F32),
            pltpu.VMEM((3, 2, HOPS, 192, lanes), F32),
            pltpu.VMEM((2, 2, 48, lanes), F32),
            pltpu.VMEM((2, 24, lanes), F32),
            pltpu.VMEM((2, 2, HOPS, 48, lanes), F32),
            pltpu.VMEM((sum_rows, 8, lanes), F32),
            pltpu.SemaphoreType.DMA((5, 2, 3)),
            pltpu.SemaphoreType.DMA((5, 2, 3)),
            pltpu.SemaphoreType.DMA((5, 2, 3)),
            pltpu.SemaphoreType.DMA((5, 2, 3)),
            pltpu.SemaphoreType.DMA((5,)),
            pltpu.SemaphoreType.DMA((5,)),
            pltpu.SemaphoreType.DMA((5,)),
            pltpu.SemaphoreType.DMA((5,)),
            pltpu.SemaphoreType.DMA((sum_rows,)),
            pltpu.SemaphoreType.DMA((sum_rows,)),
        ],
        compiler_params=pltpu.CompilerParams(collective_id=0, has_side_effects=True),
    )(right_side, counts, neighbours)
    return out[0], out[1], out[2][0, 0]


def solution(mesh):
    sizes = tuple(mesh.shape[name] for name in AXES)
    in_specs = (P(None, AXES), P(), P(None, AXES))
    out_specs = (P(None, AXES), P(None, AXES), P())
    return jax.shard_map(
        functools.partial(local, sizes), mesh=mesh, in_specs=in_specs, out_specs=out_specs, check_vma=False
    )
```

```python
import functools

import jax
import jax.numpy as jnp
from jax import lax
from jax.experimental import pallas as pl
from jax.experimental.pallas import tpu as pltpu
from jax.sharding import PartitionSpec as P

MIN_LIVE = 96
LAYER = 256
HOPS = 3
AXES = ("curve", "level")
MESH = pl.DeviceIdType.MESH
RELAXATION = 2.0 / 3.0
RELAX_FINE = RELAXATION / 6.0
RELAX_COARSE = RELAXATION / 1.5
F32 = jnp.float32


def kernel(
    sizes,
    stages,
    right_ref,
    counts_ref,
    neighbours_ref,
    solution_ref,
    residual_ref,
    norm_ref,
    source,
    first,
    second,
    image,
    zghost,
    paired,
    coarse,
    shifted,
    doubled,
    held,
    applied_ref,
    faces_fine,
    packed_fine,
    windows_fine,
    faces_coarse,
    packed_coarse,
    windows_coarse,
    sums,
    *sems,
):
    link_sems, relay_sems, pair_sems, far_sems, (sum_send, sum_recv) = [
        sems[i : i + 2] for i in range(0, 10, 2)
    ]
    curve_size, level_size = sizes
    total = curve_size * level_size
    me = lax.axis_index("curve") * level_size + lax.axis_index("level")
    lanes = right_ref.shape[1]
    half = lanes // 2

    def place(index):
        return (index // level_size, index % level_size)

    barrier = pltpu.get_barrier_semaphore()
    greeted = 0
    for size, _, peer in stages:
        for k in range(1, size):
            pl.semaphore_signal(barrier, inc=1, device_id=peer(k), device_id_type=MESH)
            greeted += 1
    direct = len(stages) == 1
    if not direct:
        for hop in range(1, HOPS + 1):
            for sign in (1, -1):
                target = (me + sign * hop + total) % total
                pl.semaphore_signal(barrier, inc=1, device_id=place(target), device_id_type=MESH)
                greeted += 1

    lane = lax.broadcasted_iota(jnp.int32, (1, lanes), 1)
    own_count = counts_ref[me]
    live = lane < own_count
    for x in range(8):
        rows = pl.ds(64 * x, 64)
        value = jnp.where(live, right_ref[rows, :], 0.0)
        source[rows, :] = value
        first[rows, :] = RELAX_FINE * value

    nb = neighbours_ref[...]
    present = nb >= 0
    owner = nb // lanes
    offset = nb % lanes
    face_id = lax.broadcasted_iota(jnp.int32, nb.shape, 0)
    hop_of = jnp.where(face_id % 2 == 0, me - owner, owner - me)
    hop_of = jnp.where(present, hop_of, -1)
    far_count = counts_ref[jnp.maximum(me - HOPS, 0)]
    odd = me % 2
    even = 1 - odd
    partner = me + 1 - 2 * odd
    earlier_pair = me >= 2
    later_pair = me - odd + 2 < total
    reaches = (1 + 2 * even, 1 + 2 * odd)
    arrives = (2 * odd, 2 * even)
    far_there = jnp.where(odd == 1, me + HOPS < total, me >= HOPS)
    far_device = (me + HOPS * (2 * odd - 1) + total) % total
    skipped = jnp.where(
        (face_id % 2 == 0) & (hop_of == HOPS), even * (far_count - half), 0
    )
    where_at = jnp.clip(offset - skipped, 0, lanes - 1)
    low_half = jnp.broadcast_to(lane < half, (8, lanes))
    pack_index = jnp.broadcast_to(odd * (own_count - half) + lane % half, (8, lanes))

    def pick(block, index):
        return jnp.take_along_axis(block, index, axis=1, mode="promise_in_bounds")

    finishing = []

    def send(src, dst, sems, at, target, sends):
        made = pltpu.make_async_remote_copy(
            src_ref=src,
            dst_ref=dst,
            send_sem=sems[0].at[at],
            recv_sem=sems[1].at[at],
            device_id=place(target),
            device_id_type=MESH,
        )
        finishing.append((made, sends))
        return made

    def exchange(stage, values, extent, faces, packed, windows, meanwhile):
        area = extent * extent
        last = extent - 1
        pack = 3 * area // 2
        for direction in (0, 1):
            at = last if direction == 0 else 0
            faces[direction, 0:area, :] = values[pl.ds(at * area, area), :]
            for x in range(extent):
                faces[direction, pl.ds(area + x * extent, extent), :] = values[
                    pl.ds(x * area + at * extent, extent), :
                ]
            faces[direction, pl.ds(2 * area, area), :] = values[pl.ds(at, area, extent), :]
        if stage == 0:
            pl.semaphore_wait(barrier, greeted)
        links = []
        for chunk in range(3):
            rows = pl.ds(chunk * area, area)
            for direction in (0, 1):
                reach = reaches[direction]
                target = me + reach if direction == 0 else me - reach
                made = send(
                    faces.at[direction, rows],
                    windows.at[direction, reach - 1, rows],
                    link_sems,
                    (stage, direction, chunk),
                    (target + total) % total,
                    later_pair if direction == 0 else earlier_pair,
                )
                pl.when(later_pair if direction == 0 else earlier_pair)(made.start)
                links.append((direction, chunk, rows, made))
        inside = send(faces.at[odd], windows.at[odd, 0], pair_sems, (stage,), partner, None)
        inside.start()
        for r in range(0, pack, 8):
            a = pick(faces[1 - odd, pl.ds(r, 8), :], pack_index)
            b = pick(faces[1 - odd, pl.ds(pack + r, 8), :], pack_index)
            packed[pl.ds(r, 8), :] = jnp.where(low_half, a, b)
        far = send(
            packed, windows.at[1 - odd, 2, pl.ds(0, pack)], far_sems, (stage,), far_device, far_there
        )
        pl.when(far_there)(far.start)
        def ghost(face, hops_in, blocks):
            direction, slot = face % 2, face // 2
            at = jnp.broadcast_to(where_at[face : face + 1, :], (8, lanes))
            is_packed = odd == direction
            at_high = jnp.where(is_packed, jnp.minimum(at + half, lanes - 1), at)
            hops = jnp.broadcast_to(hop_of[face : face + 1, :], (8, lanes))
            pieces = []
            for r in range(0, area, 8):
                row = slot * area + r
                block = blocks[r // 8]
                for hop in hops_in:
                    index = at
                    if hop == 0:
                        window = faces[direction, pl.ds(row, 8), :]
                    elif hop < HOPS or row < pack:
                        window = windows[direction, hop - 1, pl.ds(row, 8), :]
                    else:
                        start = pl.multiple_of(row - jnp.where(is_packed, pack, 0), 8)
                        window = windows[direction, hop - 1, pl.ds(start, 8), :]
                        index = at_high
                    block = jnp.where(hops == hop, pick(window, index), block)
                pieces.append(block)
            return pieces

        empty = [jnp.zeros((8, lanes), F32)] * (area // 8)
        for face in range(6):
            for r, block in enumerate(ghost(face, (0,), empty)):
                held[face, pl.ds(8 * r, 8), :] = block
        meanwhile()
        relays = []
        for direction, chunk, rows, made in links:
            comes = earlier_pair if direction == 0 else later_pair
            relay = send(
                windows.at[direction, arrives[direction], rows],
                windows.at[direction, 1, rows],
                relay_sems,
                (stage, direction, chunk),
                partner,
                comes,
            )

            @pl.when(comes)
            def _():
                made.wait_recv()
                relay.start()

            relays.append((relay, comes))
        inside.wait_recv()
        pl.when(far_there)(far.wait_recv)
        ghosts = []
        for face in range(6):
            relay, comes = relays[face]
            pl.when(comes)(relay.wait_recv)
            blocks = [held[face, pl.ds(r, 8), :] for r in range(0, area, 8)]
            ghosts.append(jnp.concatenate(ghost(face, (1, 2, 3), blocks), axis=0))
        return ghosts

    zrow = lax.broadcasted_iota(jnp.int32, (8, 8, lanes), 1)

    zghost[...] = jnp.zeros_like(zghost)

    def inner(values):
        for x in range(8):
            rows = pl.ds(64 * x, 64)
            here = values[rows, :]
            edge = jnp.zeros((8, lanes), F32)
            beside = jnp.concatenate([edge, here[:-8]], axis=0) + jnp.concatenate(
                [here[8:], edge], axis=0
            )
            if x > 0:
                beside = beside + values[pl.ds(64 * (x - 1), 64), :]
            if x < 7:
                beside = beside + values[pl.ds(64 * (x + 1), 64), :]
            cube = here.reshape(8, 8, lanes)
            below = jnp.where(zrow == 0, 0.0, pltpu.roll(cube, 1, 1))
            above = jnp.where(zrow == 7, 0.0, pltpu.roll(cube, 7, 1))
            beside = beside + (below + above).reshape(64, lanes)
            applied_ref[rows, :] = 6.0 * here - beside

    def fine(values, ghosts, use):
        g0, g1, g2, g3, g4, g5 = ghosts
        zghost[pl.ds(0, 64, 8), :] = g4
        zghost[pl.ds(7, 64, 8), :] = g5
        for x in range(8):
            rows = pl.ds(64 * x, 64)
            applied = applied_ref[rows, :] - zghost[rows, :]
            if x == 0:
                applied = applied - g0
            if x == 7:
                applied = applied - g1
            applied = jnp.concatenate(
                [
                    applied[:8] - g2[8 * x : 8 * x + 8],
                    applied[8:56],
                    applied[56:] - g3[8 * x : 8 * x + 8],
                ],
                axis=0,
            )
            use(x, rows, values[rows, :], applied)

    def exchange_fine(stage, k, values):
        return exchange(
            stage,
            values,
            8,
            faces_fine.at[k],
            packed_fine.at[k],
            windows_fine.at[k],
            lambda: inner(values),
        )

    def exchange_coarse(stage, k, meanwhile):
        return exchange(
            stage,
            coarse,
            4,
            faces_coarse.at[k],
            packed_coarse.at[k],
            windows_coarse.at[k],
            meanwhile,
        )

    def sweep(x, rows, here, applied):
        second[rows, :] = here + RELAX_FINE * (source[rows, :] - applied)

    fine(first, exchange_fine(0, 0, first), sweep)

    slabs = []

    def restrict(x, rows, here, applied):
        slabs.append(source[rows, :] - applied)
        if x % 2 == 1:
            both = slabs[x - 1] + slabs[x]
            for y in range(4):
                paired[pl.ds(32 * (x // 2) + 8 * y, 8), :] = (
                    both[16 * y : 16 * y + 8] + both[16 * y + 8 : 16 * y + 16]
                )

    ghosts = exchange_fine(1, 1, second)
    fine(second, ghosts, restrict)
    coarse_rhs = 0.125 * (paired[pl.ds(0, 64, 2), :] + paired[pl.ds(1, 64, 2), :])
    coarse_one = RELAX_COARSE * coarse_rhs
    coarse[...] = coarse_one
    g0, g1, g2, g3, g4, g5 = exchange_coarse(2, 0, lambda: None)
    beside = jnp.concatenate([g0, coarse_one[:-16]], axis=0) + jnp.concatenate(
        [coarse_one[16:], g1], axis=0
    )
    for k, shift in enumerate((4, 60, 1, 63)):
        shifted[k, :, :] = pltpu.roll(coarse_one, shift, 0)
    for x in range(4):
        shifted[0, pl.ds(16 * x, 4), :] = g2[4 * x : 4 * x + 4]
        shifted[1, pl.ds(16 * x + 12, 4), :] = g3[4 * x : 4 * x + 4]
    for x in range(4):
        for y in range(4):
            at = 16 * x + 4 * y
            shifted[2, pl.ds(at, 1), :] = g4[4 * x + y : 4 * x + y + 1]
            shifted[3, pl.ds(at + 3, 1), :] = g5[4 * x + y : 4 * x + y + 1]
    beside = beside + (shifted[0] + shifted[1]) + (shifted[2] + shifted[3])
    coarse_two = coarse_one + RELAX_COARSE * (coarse_rhs - 0.25 * (6.0 * coarse_one - beside))
    coarse[...] = coarse_two
    paired[pl.ds(0, 64, 2), :] = coarse_two
    paired[pl.ds(1, 64, 2), :] = coarse_two

    def correct():
        for x in range(8):
            for y in range(8):
                rows = pl.ds(64 * x + 8 * y, 8)
                lift = paired[pl.ds(32 * (x // 2) + 8 * (y // 2), 8), :]
                second[rows, :] = second[rows, :] + lift
        inner(second)

    corrections = exchange_coarse(3, 1, correct)
    for face in range(6):
        doubled[face, pl.ds(0, 16, 2), :] = corrections[face]
        doubled[face, pl.ds(1, 16, 2), :] = corrections[face]
        ghosts[face] = ghosts[face] + jnp.concatenate(
            [doubled[face, pl.ds(8 * (a // 2), 8), :] for a in range(8)], axis=0
        )

    def smooth(x, rows, here, applied):
        first[rows, :] = here + RELAX_FINE * (source[rows, :] - applied)

    fine(second, ghosts, smooth)

    parts = [jnp.zeros((8, lanes), F32)] * 5

    def fold(block):
        return jnp.sum(block.reshape(8, 8, lanes), axis=0)

    def finish(x, rows, here, applied):
        image[rows, :] = applied
        r = source[rows, :]
        for k, term in enumerate((r * here, here * applied, r * r, r * applied, applied * applied)):
            parts[k] = parts[k] + fold(term)

    fine(first, exchange_fine(4, 2, first), finish)

    tile = jnp.zeros((1, lanes), F32)
    for k in range(5):
        one = jnp.sum(jnp.sum(parts[k], axis=0, keepdims=True), axis=1, keepdims=True)
        tile = jnp.where(lane == k, one, tile)
    base = 0
    for size, mine, peer in stages:
        sums[base + mine] = tile
        copies = []
        for k in range(1, size):
            made = pltpu.make_async_remote_copy(
                src_ref=sums.at[base + mine],
                dst_ref=sums.at[base + mine],
                send_sem=sum_send.at[base + k],
                recv_sem=sum_recv.at[base + k],
                device_id=peer(k),
                device_id_type=MESH,
            )
            made.start()
            copies.append(made)
        for made in copies:
            made.wait_recv()
        tile = jnp.sum(sums[base : base + size], axis=0)
        for made in copies:
            made.wait_send()
        base += size
    along, curvature, old_square, cross, image_square = [
        jnp.sum(jnp.where(lane == k, tile, 0.0), axis=1, keepdims=True) for k in range(5)
    ]
    step = along / curvature
    square = old_square - 2.0 * step * cross + step * step * image_square
    norm_ref[0] = jnp.sqrt(square)[0, 0]
    for x in range(8):
        rows = pl.ds(64 * x, 64)
        solution_ref[rows, :] = step * first[rows, :]
        residual_ref[rows, :] = source[rows, :] - step * image[rows, :]
    for made, sends in finishing:
        if sends is None:
            made.wait_send()
        else:
            pl.when(sends)(made.wait_send)


def local(sizes, right_side, counts, neighbours):
    cells, lanes = right_side.shape
    curve_size, level_size = sizes
    total = curve_size * level_size

    def body(*refs):
        curve, level = lax.axis_index("curve"), lax.axis_index("level")
        if total <= 64:
            me = curve * level_size + level

            def everyone(k):
                other = (me + k) % total
                return (other // level_size, other % level_size)

            stages = [(total, me, everyone)]
        else:
            stages = [
                (level_size, level, lambda k: (curve, (level + k) % level_size)),
                (curve_size, curve, lambda k: ((curve + k) % curve_size, level)),
            ]
        kernel(sizes, stages, *refs)

    sum_rows = total if total <= 64 else curve_size + level_size
    vmem = pl.BlockSpec(memory_space=pltpu.VMEM)
    block = jax.ShapeDtypeStruct((cells, lanes), F32)
    out = pl.pallas_call(
        body,
        out_shape=(block, block, jax.ShapeDtypeStruct((1,), F32)),
        in_specs=[vmem, pl.BlockSpec(memory_space=pltpu.SMEM), vmem],
        out_specs=(vmem, vmem, pl.BlockSpec(memory_space=pltpu.SMEM)),
        scratch_shapes=[
            pltpu.VMEM((cells, lanes), F32),
            pltpu.VMEM((cells, lanes), F32),
            pltpu.VMEM((cells, lanes), F32),
            pltpu.VMEM((cells, lanes), F32),
            pltpu.VMEM((cells, lanes), F32),
            pltpu.VMEM((cells // 4, lanes), F32),
            pltpu.VMEM((cells // 8, lanes), F32),
            pltpu.VMEM((4, cells // 8, lanes), F32),
            pltpu.VMEM((6, 32, lanes), F32),
            pltpu.VMEM((6, 64, lanes), F32),
            pltpu.VMEM((cells, lanes), F32),
            pltpu.VMEM((3, 2, 192, lanes), F32),
            pltpu.VMEM((3, 96, lanes), F32),
            pltpu.VMEM((3, 2, HOPS, 192, lanes), F32),
            pltpu.VMEM((2, 2, 48, lanes), F32),
            pltpu.VMEM((2, 24, lanes), F32),
            pltpu.VMEM((2, 2, HOPS, 48, lanes), F32),
            pltpu.VMEM((sum_rows, 1, lanes), F32),
            pltpu.SemaphoreType.DMA((5, 2, 3)),
            pltpu.SemaphoreType.DMA((5, 2, 3)),
            pltpu.SemaphoreType.DMA((5, 2, 3)),
            pltpu.SemaphoreType.DMA((5, 2, 3)),
            pltpu.SemaphoreType.DMA((5,)),
            pltpu.SemaphoreType.DMA((5,)),
            pltpu.SemaphoreType.DMA((5,)),
            pltpu.SemaphoreType.DMA((5,)),
            pltpu.SemaphoreType.DMA((sum_rows,)),
            pltpu.SemaphoreType.DMA((sum_rows,)),
        ],
        compiler_params=pltpu.CompilerParams(collective_id=0, has_side_effects=True),
    )(right_side, counts, neighbours)
    return out[0], out[1], out[2].reshape(())


def solution(mesh):
    sizes = tuple(mesh.shape[name] for name in AXES)
    in_specs = (P(None, AXES), P(), P(None, AXES))
    out_specs = (P(None, AXES), P(None, AXES), P())
    return jax.shard_map(
        functools.partial(local, sizes), mesh=mesh, in_specs=in_specs, out_specs=out_specs, check_vma=False
    )
```
